512 devices in a mesh: lat: 16 (over y_lo, z), lon: 32 (over x, y_hi, core).
Axes of the slice: x: 4, y: 8 (y_hi: 4, y_lo: 2; y = y_hi * 2 + y_lo), z: 8, core: 2. Of those that a mesh axis runs over, the one named last changes fastest.
Arguments:
- tokens: bfloat16 [384, 256, 768], P('lat', 'lon'), may hold values from -6 to 6
- gain_zonal: float32 [768], replicated, may hold values from 0.25 to 1.75
- qkv_zonal: bfloat16 [768, 2304], P('lat'), may hold values from -1 to 1
- out_zonal: bfloat16 [768, 768], P('lat'), may hold values from -0.21875 to 0.21875
- gain_merid: float32 [768], replicated, may hold values from 0.25 to 1.75
- qkv_merid: bfloat16 [768, 2304], P('lat'), may hold values from -1 to 1
- out_merid: bfloat16 [768, 768], P('lat'), may hold values from -0.21875 to 0.21875
Outputs:
- result: bfloat16 [384, 256, 768], P('lat', 'lon')
The draws below stay inside these ranges and needn't reach their ends.
All inputs are finite; a program needn't handle non-finite values.
Results may differ from the reference program's by a relative error of at most 0.0095.
Values may be sent and summed in bfloat16 or wider, within the bound.
A program may use at most 64 MiB of HBM per device.

```python
import jax
import jax.numpy as jnp
from jax import lax

HEAD_DIM = 64
D = 768
NLAT = 384
NLON = 256


def projection_noise(key, salt):
    noise = jax.random.truncated_normal(jax.random.fold_in(key, salt), -4.0, 4.0, (D, 3 * D), jnp.float32)
    return noise * D ** (-0.5)


def draw_tokens(key, part):
    noise = jax.random.truncated_normal(jax.random.fold_in(key, 7003), -6.0, 6.0, (NLAT, NLON, D), jnp.float32)
    return noise.astype(jnp.bfloat16)


def draw_qkv_zonal(key, part):
    noise = projection_noise(key, 7101)
    return noise.astype(jnp.bfloat16)


def draw_qkv_merid(key, part):
    noise = projection_noise(key, 7201)
    return noise.astype(jnp.bfloat16)


def level_of(own_key, dims, shards, smallest, top_value):
    def one(dim, shards_of):
        heights = jax.random.uniform(jax.random.fold_in(jax.random.fold_in(own_key, 6), dim), (shards_of,), jnp.float32, smallest / len(shards), top_value / len(shards))
        return jnp.repeat(jnp.exp(heights), dims[dim] // shards_of).reshape((-1,) + (1,) * (len(dims) - dim - 1))

    level = one(*shards[0])
    for cut in shards[1:]:
        level = level * one(*cut)
    return level


def normal_values(key, shape, scale, limit, pieces=(), kind=jnp.bfloat16):
    entries = scale * jax.random.normal(key, shape, jnp.float32)
    if pieces:
        entries = entries * level_of(key, shape, pieces, -0.22, 0.18)
    return jnp.clip(entries, -limit, limit).astype(kind)


def setup_inputs(seed: int = 0) -> dict:
    streams_of = jax.random.split(jax.random.key(seed), 8)
    tokens = draw_tokens(jax.random.fold_in(streams_of[7], 71), 0)
    gain_zonal = jnp.clip(1.0 + 0.15 * jax.random.normal(streams_of[1], (D,), jnp.float32), 0.25, 1.75)
    qkv_zonal = draw_qkv_zonal(jax.random.fold_in(streams_of[7], 71), 0)
    out_zonal = normal_values(streams_of[3], (D, D), D ** -0.5, 0.21875, ((0, 16),))
    gain_merid = jnp.clip(1.0 + 0.15 * jax.random.normal(streams_of[4], (D,), jnp.float32), 0.25, 1.75)
    qkv_merid = draw_qkv_merid(jax.random.fold_in(streams_of[7], 71), 0)
    out_merid = normal_values(streams_of[6], (D, D), D ** -0.5, 0.21875, ((0, 16),))
    return dict(tokens=tokens, gain_zonal=gain_zonal, qkv_zonal=qkv_zonal, out_zonal=out_zonal, gain_merid=gain_merid, qkv_merid=qkv_merid, out_merid=out_merid)


def normalize(values, gain):
    wide = values.astype(jnp.float32)
    factor = lax.rsqrt(lax.optimization_barrier(jnp.mean(wide * wide, axis=-1, keepdims=True)) + 1e-05)
    return (wide * factor * gain).astype(jnp.bfloat16)

def attend(fields):
    count, length, width = fields.shape
    model = width // 3
    heads = model // HEAD_DIM
    split = fields.reshape(count, length, 3, heads, HEAD_DIM)
    stacked = jnp.moveaxis(split, (3, 2), (0, 1))

    def one_head(parts):
        query = parts[0].astype(jnp.float32)
        keys = parts[1].astype(jnp.float32)
        values = parts[2].astype(jnp.float32)
        scores = jnp.einsum('rqe,rke->rqk', query, keys) * HEAD_DIM ** (-0.5)
        ceiling = lax.optimization_barrier(jnp.max(scores, axis=-1, keepdims=True))
        powers = jnp.exp(scores - ceiling)
        weights = (powers / lax.optimization_barrier(jnp.sum(powers, axis=-1, keepdims=True))).astype(jnp.bfloat16)
        mixed = jnp.einsum('rqk,rke->rqe', weights.astype(jnp.float32), values)
        return mixed.astype(jnp.bfloat16)
    outputs = lax.map(one_head, stacked)
    return jnp.moveaxis(outputs, 0, 2).reshape(count, length, model)

def section(lines, gain, qkv_weight, out_weight):

    def one_line(line):
        normed = normalize(line, gain)
        fields = jnp.dot(normed, qkv_weight, preferred_element_type=jnp.float32).astype(jnp.bfloat16)
        mixed = attend(fields[None])[0]
        update = jnp.dot(mixed, out_weight, preferred_element_type=jnp.float32)
        return (line.astype(jnp.float32) + update).astype(jnp.bfloat16)
    return lax.map(one_line, lines)

def reference(tokens, gain_zonal, qkv_zonal, out_zonal, gain_merid, qkv_merid, out_merid):
    after_zonal = section(tokens, gain_zonal, qkv_zonal, out_zonal)
    columns = jnp.swapaxes(after_zonal, 0, 1)
    result = section(columns, gain_merid, qkv_merid, out_merid)
    return jnp.swapaxes(result, 0, 1)
```

```python
import functools

import jax
import jax.numpy as jnp
from jax import lax
from jax.experimental import pallas as pl
from jax.experimental.pallas import tpu as pltpu
from jax.sharding import PartitionSpec as P

MESH = pl.DeviceIdType.MESH
F32 = jnp.float32
BF16 = jnp.bfloat16
EPS = 1e-05
NX, NG, NZ, NY = 4, 8, 8, 2


def norm(values, gain):
    factor = lax.rsqrt(jnp.mean(values * values, axis=-1, keepdims=True) + EPS)
    return (values * factor * gain).astype(BF16)


def matmul(a, b):
    return jnp.dot(a, b, preferred_element_type=F32)


def weights_of(query, keys):
    scores = lax.dot_general(query, keys, (((1,), (1,)), ((), ())), preferred_element_type=F32) * 0.125
    powers = jnp.exp(scores - jnp.max(scores, axis=-1, keepdims=True))
    return (powers * (1.0 / jnp.sum(powers, axis=-1, keepdims=True))).astype(BF16)


def kernel(
    tok, gz, wz_in, oz_in, gm, wm_in, om_in, out,
    wz_s, wm_s, wz, oz, wm, om, t_buf, h_buf, s_buf, u_buf, h2_buf, mz, mm, after,
    w_sem, a_sem, b_sem, c_sem, d_sem, send,
):
    lat, lon = lax.axis_index("lat"), lax.axis_index("lon")
    yl, z = lat // NZ, lax.rem(lat, NZ)
    x, g = lon // NG, lax.rem(lon, NG)
    yh, c = g // 2, lax.rem(g, 2)
    sibling = lon + 1 - 2 * c
    pair = (1 - yl) * NZ + z

    def remote(src, dst, ssem, rsem, to_lat, to_lon):
        return pltpu.make_async_remote_copy(
            src_ref=src, dst_ref=dst, send_sem=ssem, recv_sem=rsem,
            device_id=(to_lat, to_lon), device_id_type=MESH,
        )

    def local(src, dst, sem):
        return pltpu.make_async_copy(src, dst, sem)

    barrier = pltpu.get_barrier_semaphore()

    @pl.loop(1, NX * NG)
    def _(k):
        pl.semaphore_signal(barrier, inc=1, device_id=(lat, lax.rem(lon + k, NX * NG)), device_id_type=MESH)

    @pl.loop(1, NY * NZ)
    def _(k):
        pl.semaphore_signal(barrier, inc=1, device_id=(lax.rem(lat + k, NY * NZ), lon), device_id_type=MESH)

    for i in range(NX):
        @pl.when(x == i)
        def _():
            rows = wz_in[...].astype(F32)
            def part(t, low, high):
                return rows[:, 768 * t + 192 * i + low : 768 * t + 192 * i + high]
            wz_s[:, 0:128] = part(0, 0, 128).astype(BF16)
            wz_s[:, 128:256] = part(1, 0, 128).astype(BF16)
            wz_s[:, 256:384] = part(2, 0, 128).astype(BF16)
            wz_s[:, 384:512] = jnp.concatenate([part(2, 128, 192), part(0, 128, 192)], axis=1).astype(BF16)
            wz_s[:, 512:640] = jnp.concatenate([jnp.zeros((48, 64), F32), part(1, 128, 192)], axis=1).astype(BF16)
    for h in range(2):
        for t in range(3):
            wm_s[h, :, 384 * t : 384 * t + 384] = wm_in[:, 768 * t + 384 * h : 768 * t + 384 * h + 384]

    pl.semaphore_wait(barrier, NX * NG - 1 + NY * NZ - 1)

    near = [(0, 1), (2, 0), (2, 1), (1, 0), (3, 0), (1, 1), (3, 1)]

    def place(dy, dc):
        return lax.rem(yh + dy, 4) * 2 + lax.rem(c + dc, 2)

    own_rows = pl.ds(3 * g, 3)
    local(tok.at[own_rows], t_buf.at[x, g], a_sem.at[lon]).start()
    for dy, dc in near:
        to = place(dy, dc)
        remote(tok.at[pl.ds(3 * to, 3)], t_buf.at[x, g], send.at[0], a_sem.at[lon], lat, x * NG + to).start()

    emits_z = lax.rem(z, 2) == c

    @pl.when(emits_z)
    def _():
        local(wz_s, wz.at[pl.ds(48 * lat, 48)], w_sem.at[0, lat]).start()

        @pl.loop(1, NY * NZ)
        def _(k):
            remote(wz_s, wz.at[pl.ds(48 * lat, 48)], send.at[1], w_sem.at[0, lat], lax.rem(lat + k, NY * NZ), lon).start()

    def onward(source, src):
        for dx in (1, 3, 2):
            remote(src, t_buf.at[x, source], send.at[2], a_sem.at[x * NG + source], lat, lax.rem(x + dx, NX) * NG + g).start()

    onward(g, tok.at[own_rows])
    for dy, dc in [(0, 1), (1, 0), (3, 0), (1, 1), (3, 1), (2, 0), (2, 1)]:
        source = place(dy, dc)
        local(t_buf.at[x, source], t_buf.at[x, source], a_sem.at[x * NG + source]).wait()
        onward(source, t_buf.at[x, source])

    @pl.loop(0, NZ)
    def _(k):
        source = (k // 4) * NZ + 2 * lax.rem(k, 4) + c
        block = wz.at[pl.ds(48 * source, 48)]
        local(block, block, w_sem.at[0, source]).wait()
        remote(block, block, send.at[3], w_sem.at[0, source], lat, sibling).start()

    emits = z == 2 * x + c
    packs = ((1, oz_in, oz, 4), (2, wm_s, wm, 6), (3, om_in, om, 8))

    @pl.when(emits)
    def _():
        for p, src, dst, s in packs:
            block = dst.at[pl.ds(48 * lat, 48)]
            local(src.at[yl] if p == 2 else src, block, w_sem.at[p, lat]).start()

            @pl.loop(1, NY * NZ)
            def _(k):
                to = lax.rem(lat + k, NY * NZ)
                piece = src.at[to // NZ] if p == 2 else src
                remote(piece, block, send.at[s], w_sem.at[p, lat], to, lon).start()

    def relay(p, dst, s):
        for y in range(NY):
            source = y * NZ + 2 * x + c
            block = dst.at[pl.ds(48 * source, 48)]
            local(block, block, w_sem.at[p, source]).wait()
            for dx in (1, 3, 2):
                remote(block, block, send.at[s + 1], w_sem.at[p, source], lat, lax.rem(x + dx, NX) * NG + g).start()
            remote(block, block, send.at[s + 1], w_sem.at[p, source], lat, sibling).start()

    def share(p, dst, s):
        for dx in (1, 3, 2):
            for y in range(NY):
                source = y * NZ + 2 * lax.rem(x + dx, NX) + c
                block = dst.at[pl.ds(48 * source, 48)]
                local(block, block, w_sem.at[p, source]).wait()
                remote(block, block, send.at[s + 1], w_sem.at[p, source], lat, sibling).start()

    def settle(p, dst):
        @pl.loop(0, NZ)
        def _(k):
            source = (k // 4) * NZ + 2 * lax.rem(k, 4) + 1 - c
            block = dst.at[pl.ds(48 * source, 48)]
            local(block, block, w_sem.at[p, source]).wait()

    relay(1, oz, 4)

    for dx in (1, 3, 2):
        @pl.loop(0, NG)
        def _(k):
            place_x = lax.rem(x + dx, NX)
            block = t_buf.at[place_x, k]
            local(block, block, a_sem.at[place_x * NG + k]).wait()
    local(t_buf.at[x, g], t_buf.at[x, g], a_sem.at[lon]).wait()
    settle(0, wz)

    low256 = lax.broadcasted_iota(jnp.int32, (256, 128), 1) < 64
    zero256 = jnp.zeros((256, 128), BF16)

    @pl.loop(0, 3)
    def _(r):
        values = t_buf[:, :, r].astype(F32).reshape(256, 768)
        normed = norm(values, gz[...])
        fields = matmul(normed, wz[...]).astype(BF16)
        q, k, v = fields[:, 0:128], fields[:, 128:256], fields[:, 256:384]
        vq, pad_k = fields[:, 384:512], fields[:, 512:640]
        m0 = matmul(weights_of(q, jnp.where(low256, k, zero256)), v)
        m1 = matmul(weights_of(q, jnp.where(low256, zero256, k)), v)
        m2 = matmul(weights_of(vq, pad_k), vq)
        mz[:, pl.ds(r, 1), :, 0:128] = jnp.where(low256, m0, m1).reshape(32, 1, 8, 128).astype(BF16)
        mz[:, pl.ds(r, 1), :, 128:192] = m2[:, 0:64].reshape(32, 1, 8, 64).astype(BF16)

    local(mz.at[lon], h_buf.at[x, own_rows], b_sem.at[lon]).start()

    @pl.loop(1, NX * NG)
    def _(k):
        to = lax.rem(lon + k, NX * NG)
        remote(mz.at[to], h_buf.at[x, own_rows], send.at[10], b_sem.at[lon], lat, to).start()

    share(1, oz, 4)
    relay(2, wm, 6)
    settle(1, oz)

    @pl.loop(0, NX * NG)
    def _(k):
        block = h_buf.at[k // NG, pl.ds(3 * lax.rem(k, NG), 3)]
        local(block, block, b_sem.at[k]).wait()

    total = tok[...].astype(F32).reshape(192, 768)
    for i in range(NX):
        mixed = h_buf[i].astype(F32).reshape(192, 192).astype(BF16)
        total += matmul(mixed, oz[192 * i : 192 * i + 192, :])
    by_row = total.astype(BF16)
    ii = lax.broadcasted_iota(jnp.int32, (192, 192), 1)
    jj = lax.broadcasted_iota(jnp.int32, (192, 192), 0)
    turn = jnp.where((ii & 7) * 24 + (ii >> 3) == jj, 1.0, 0.0).astype(BF16)
    by_col = matmul(turn, by_row)
    after[...] = by_col
    s_buf[...] = by_col.reshape(8, 3, 8, 768).astype(BF16)

    local(s_buf.at[z], u_buf.at[yl, z], c_sem.at[lat]).start()
    for dz in (4, 3, 5, 2, 6, 1, 7):
        to = lax.rem(z + dz, NZ)
        remote(s_buf.at[to], u_buf.at[yl, z], send.at[11], c_sem.at[lat], yl * NZ + to, lon).start()
    remote(s_buf.at[z], u_buf.at[yl, z], send.at[12], c_sem.at[lat], pair, lon).start()
    for dz in (1, 7, 2, 6, 3, 5, 4):
        source = lax.rem(z + dz, NZ)
        block = u_buf.at[yl, source]
        local(block, block, c_sem.at[yl * NZ + source]).wait()
        remote(block, block, send.at[12], c_sem.at[yl * NZ + source], pair, lon).start()

    share(2, wm, 6)
    relay(3, om, 8)
    settle(2, wm)

    local(u_buf.at[yl, z], u_buf.at[yl, z], c_sem.at[lat]).wait()

    @pl.loop(0, NZ)
    def _(k):
        block = u_buf.at[1 - yl, k]
        local(block, block, c_sem.at[(1 - yl) * NZ + k]).wait()

    low384 = lax.broadcasted_iota(jnp.int32, (384, 128), 1) < 64
    zero384 = jnp.zeros((384, 128), BF16)
    normed = norm(u_buf[...].astype(F32).reshape(384, 768), gm[...])
    for j in range(3):
        at = 128 * j
        q = matmul(normed, wm[:, at : at + 128]).astype(BF16)
        k = matmul(normed, wm[:, 384 + at : 512 + at]).astype(BF16)
        v = matmul(normed, wm[:, 768 + at : 896 + at]).astype(BF16)
        m0 = matmul(weights_of(q, jnp.where(low384, k, zero384)), v)
        m1 = matmul(weights_of(q, jnp.where(low384, zero384, k)), v)
        mm[:, :, :, at : at + 128] = jnp.where(low384, m0, m1).reshape(16, 3, 8, 128).astype(BF16)

    local(mm.at[lat], h2_buf.at[yl, z], d_sem.at[lat]).start()

    @pl.loop(1, NY * NZ)
    def _(k):
        to = lax.rem(lat + k, NY * NZ)
        remote(mm.at[to], h2_buf.at[yl, z], send.at[13], d_sem.at[lat], to, lon).start()

    share(3, om, 8)
    settle(3, om)

    @pl.loop(0, NY * NZ)
    def _(k):
        block = h2_buf.at[k // NZ, lax.rem(k, NZ)]
        local(block, block, d_sem.at[k]).wait()

    total = after[...]
    for i in range(NY):
        mixed = h2_buf[i].astype(F32).reshape(192, 384).astype(BF16)
        total += matmul(mixed, om[384 * i : 384 * i + 384, :])
    back = jnp.where((jj & 7) * 24 + (jj >> 3) == ii, 1.0, 0.0).astype(BF16)
    out[...] = matmul(back, total.astype(BF16)).reshape(24, 8, 768).astype(BF16)

    def drain(sem, ref):
        local(ref, ref, sem).wait()

    drain(send.at[0], t_buf.at[0, pl.ds(0, NG - 1)])
    drain(send.at[2], t_buf.at[pl.ds(0, 3)])

    @pl.when(emits_z)
    def _():
        drain(send.at[1], wz.at[pl.ds(0, 720)])

    drain(send.at[3], wz.at[pl.ds(0, 384)])

    @pl.when(emits)
    def _():
        for p, src, dst, s in packs:
            drain(send.at[s], dst.at[pl.ds(0, 720)])

    for p, src, dst, s in packs:
        drain(send.at[s + 1], dst.at[pl.ds(0, 672)])
    drain(send.at[10], mz.at[pl.ds(0, NX * NG - 1)])
    drain(send.at[11], s_buf.at[pl.ds(0, NZ - 1)])
    drain(send.at[12], s_buf)
    drain(send.at[13], mm.at[pl.ds(0, NY * NZ - 1)])


def body(tokens, gain_zonal, qkv_zonal, out_zonal, gain_merid, qkv_merid, out_merid):
    return pl.pallas_call(
        kernel,
        out_shape=jax.ShapeDtypeStruct(tokens.shape, BF16),
        in_specs=[pl.BlockSpec(memory_space=pltpu.VMEM)] * 7,
        out_specs=pl.BlockSpec(memory_space=pltpu.VMEM),
        scratch_shapes=[
            pltpu.VMEM((48, 640), BF16),
            pltpu.VMEM((2, 48, 1152), BF16),
            pltpu.VMEM((768, 640), BF16),
            pltpu.VMEM((768, 768), BF16),
            pltpu.VMEM((768, 1152), BF16),
            pltpu.VMEM((768, 768), BF16),
            pltpu.VMEM((NX, NG, 3, 8, 768), BF16),
            pltpu.VMEM((NX, 24, 8, 192), BF16),
            pltpu.VMEM((8, 3, 8, 768), BF16),
            pltpu.VMEM((NY, NZ, 3, 8, 768), BF16),
            pltpu.VMEM((NY, NZ, 3, 8, 384), BF16),
            pltpu.VMEM((NX * NG, 3, 8, 192), BF16),
            pltpu.VMEM((NY * NZ, 3, 8, 384), BF16),
            pltpu.VMEM((192, 768), F32),
            pltpu.SemaphoreType.DMA((4, NY * NZ)),
            pltpu.SemaphoreType.DMA((NX * NG,)),
            pltpu.SemaphoreType.DMA((NX * NG,)),
            pltpu.SemaphoreType.DMA((NY * NZ,)),
            pltpu.SemaphoreType.DMA((NY * NZ,)),
            pltpu.SemaphoreType.DMA((14,)),
        ],
        compiler_params=pltpu.CompilerParams(
            collective_id=0, has_side_effects=True, vmem_limit_bytes=56 * 1024 * 1024
        ),
        name="axial",
    )(tokens, gain_zonal.reshape(1, -1), qkv_zonal, out_zonal, gain_merid.reshape(1, -1), qkv_merid, out_merid)


def solution(mesh):
    return jax.shard_map(
        body,
        mesh=mesh,
        in_specs=(
            P("lat", "lon", None),
            P(),
            P("lat", None),
            P("lat", None),
            P(),
            P("lat", None),
            P("lat", None),
        ),
        out_specs=P("lat", "lon", None),
        check_vma=False,
    )
```

```python
import functools

import jax
import jax.numpy as jnp
from jax import lax
from jax.experimental import pallas as pl
from jax.experimental.pallas import tpu as pltpu
from jax.sharding import PartitionSpec as P

MESH = pl.DeviceIdType.MESH
F32 = jnp.float32
BF16 = jnp.bfloat16
EPS = 1e-05
NX, NG, NZ, NY = 4, 8, 8, 2


def norm(values, gain):
    factor = lax.rsqrt(jnp.mean(values * values, axis=-1, keepdims=True) + EPS)
    return (values * factor * gain).astype(BF16)


def matmul(a, b):
    return jnp.dot(a, b, preferred_element_type=F32)


def weights_of(query, keys):
    scores = lax.dot_general(query, keys, (((1,), (1,)), ((), ())), preferred_element_type=F32) * 0.125
    powers = jnp.exp(scores - jnp.max(scores, axis=-1, keepdims=True))
    return (powers * (1.0 / jnp.sum(powers, axis=-1, keepdims=True))).astype(BF16)


def kernel(
    tok, gz, wz_in, oz_in, gm, wm_in, om_in, out,
    wz_s, wm_s, wz, oz, wm, om, t_buf, h_buf, s_buf, u_buf, h2_buf, mz, mm, after,
    w_sem, a_sem, b_sem, c_sem, d_sem, send,
):
    lat, lon = lax.axis_index("lat"), lax.axis_index("lon")
    yl, z = lat // NZ, lax.rem(lat, NZ)
    x, g = lon // NG, lax.rem(lon, NG)
    yh, c = g // 2, lax.rem(g, 2)
    sibling = lon + 1 - 2 * c
    pair = (1 - yl) * NZ + z

    def remote(src, dst, ssem, rsem, to_lat, to_lon):
        return pltpu.make_async_remote_copy(
            src_ref=src, dst_ref=dst, send_sem=ssem, recv_sem=rsem,
            device_id=(to_lat, to_lon), device_id_type=MESH,
        )

    def local(src, dst, sem):
        return pltpu.make_async_copy(src, dst, sem)

    def wait(ref, sem):
        local(ref, ref, sem).wait()

    barrier = pltpu.get_barrier_semaphore()

    @pl.loop(1, NX * NG)
    def _(k):
        pl.semaphore_signal(barrier, inc=1, device_id=(lat, lax.rem(lon + k, NX * NG)), device_id_type=MESH)

    @pl.loop(1, NY * NZ)
    def _(k):
        pl.semaphore_signal(barrier, inc=1, device_id=(lax.rem(lat + k, NY * NZ), lon), device_id_type=MESH)

    for i in range(NX):
        @pl.when(x == i)
        def _():
            rows = wz_in[...].astype(F32)
            def part(t, low, high):
                return rows[:, 768 * t + 192 * i + low : 768 * t + 192 * i + high]
            wz_s[:, 0:128] = part(0, 0, 128).astype(BF16)
            wz_s[:, 128:256] = part(1, 0, 128).astype(BF16)
            wz_s[:, 256:384] = part(2, 0, 128).astype(BF16)
            wz_s[:, 384:512] = jnp.concatenate([part(2, 128, 192), part(0, 128, 192)], axis=1).astype(BF16)
            wz_s[:, 512:640] = jnp.concatenate([jnp.zeros((48, 64), F32), part(1, 128, 192)], axis=1).astype(BF16)
    for h in range(2):
        for t in range(3):
            wm_s[h, :, 384 * t : 384 * t + 384] = wm_in[:, 768 * t + 384 * h : 768 * t + 384 * h + 384]

    pl.semaphore_wait(barrier, NX * NG - 1 + NY * NZ - 1)

    def place(dy, dc):
        return lax.rem(yh + dy, 4) * 2 + lax.rem(c + dc, 2)

    own_rows = pl.ds(3 * g, 3)
    local(tok.at[own_rows], t_buf.at[x, g], a_sem.at[lon]).start()
    for dy, dc in [(0, 1), (2, 0), (2, 1), (1, 0), (3, 0), (1, 1), (3, 1)]:
        to = place(dy, dc)
        remote(tok.at[pl.ds(3 * to, 3)], t_buf.at[x, g], send.at[0], a_sem.at[lon], lat, x * NG + to).start()

    def onward(source, src):
        for dx in (1, 3, 2):
            remote(src, t_buf.at[x, source], send.at[2], a_sem.at[x * NG + source], lat, lax.rem(x + dx, NX) * NG + g).start()

    onward(g, tok.at[own_rows])

    def rows_of(dst, source):
        return dst.at[pl.ds(48 * source, 48)]

    def along(p, dst, s, source, src, steps):
        for dz in steps:
            remote(src, rows_of(dst, source), send.at[s], w_sem.at[p, source], yl * NZ + lax.rem(z + dz, NZ), lon).start()

    def emit(p, src, dst, s):
        mine, theirs = (src.at[yl], src.at[1 - yl]) if p == 2 else (src, src)
        remote(theirs, rows_of(dst, lat), send.at[s], w_sem.at[p, lat], pair, lon).start()
        local(mine, rows_of(dst, lat), w_sem.at[p, lat]).start()
        along(p, dst, s, lat, mine, (1, 7, 2, 6))

    active = lax.rem(z, 2) == c

    @pl.when(active)
    def _():
        emit(0, wz_s, wz, 1)

    dz_own = lax.rem(z + NZ - 2 * x - c, NZ)
    source_own, source_far = yl * NZ + 2 * x + c, (1 - yl) * NZ + 2 * x + c
    packs = ((1, oz_in, oz, 4), (2, wm_s, wm, 6), (3, om_in, om, 8))

    def first(p, src, dst, s):
        @pl.when(dz_own == 0)
        def _():
            emit(p, src, dst, s)

    def second(p, src, dst, s):
        @pl.when(dz_own == 0)
        def _():
            wait(rows_of(dst, source_own), w_sem.at[p, source_own])
            wait(rows_of(dst, source_far), w_sem.at[p, source_far])
            along(p, dst, s, source_far, rows_of(dst, source_far), (1, 7, 2, 6))

    def third(p, src, dst, s):
        for at, steps in ((2, (1, 2)), (6, (7,))):
            @pl.when(dz_own == at)
            def _():
                for source in (source_own, source_far):
                    wait(rows_of(dst, source), w_sem.at[p, source])
                    along(p, dst, s, source, rows_of(dst, source), steps)

    def relay(p, src, dst, s):
        for source in (source_own, source_far):
            block = rows_of(dst, source)

            @pl.when((dz_own != 0) & (dz_own != 2) & (dz_own != 6))
            def _():
                wait(block, w_sem.at[p, source])

            for dx in (1, 3, 2):
                remote(block, block, send.at[s + 1], w_sem.at[p, source], lat, lax.rem(x + dx, NX) * NG + g).start()
            remote(block, block, send.at[s + 1], w_sem.at[p, source], lat, sibling).start()

    def share(p, src, dst, s):
        for dx in (1, 3, 2):
            for y in range(NY):
                source = y * NZ + 2 * lax.rem(x + dx, NX) + c
                block = rows_of(dst, source)
                wait(block, w_sem.at[p, source])
                remote(block, block, send.at[s + 1], w_sem.at[p, source], lat, sibling).start()

    def settle(p, dst):
        @pl.loop(0, NZ)
        def _(k):
            source = (k // 4) * NZ + 2 * lax.rem(k, 4) + 1 - c
            wait(rows_of(dst, source), w_sem.at[p, source])

    first(*packs[0])

    def pass_on(pieces):
        for dy, dc in pieces:
            source = place(dy, dc)
            wait(t_buf.at[x, source], a_sem.at[x * NG + source])
            onward(source, t_buf.at[x, source])

    pass_on([(0, 1)])

    @pl.when(active)
    def _():
        wait(rows_of(wz, pair), w_sem.at[0, pair])
        along(0, wz, 1, pair, rows_of(wz, pair), (1, 7, 2, 6))

    second(*packs[0])
    pass_on([(1, 0), (3, 0), (1, 1), (3, 1)])

    def to_sibling(source):
        block = rows_of(wz, source)
        remote(block, block, send.at[3], w_sem.at[0, source], lat, sibling).start()

    @pl.when(active)
    def _():
        for y in (yl, 1 - yl):
            for dz, steps in ((6, (1, 2)), (2, (7,))):
                source = y * NZ + lax.rem(z + dz, NZ)
                wait(rows_of(wz, source), w_sem.at[0, source])
                along(0, wz, 1, source, rows_of(wz, source), steps)
                to_sibling(source)

    third(*packs[0])
    first(*packs[1])
    pass_on([(2, 0), (2, 1)])

    @pl.when(active)
    def _():
        wait(rows_of(wz, lat), w_sem.at[0, lat])
        to_sibling(lat)
        to_sibling(pair)
        for y in (yl, 1 - yl):
            source = y * NZ + lax.rem(z + 4, NZ)
            wait(rows_of(wz, source), w_sem.at[0, source])
            to_sibling(source)

    @pl.when(jnp.logical_not(active))
    def _():
        for y in (yl, 1 - yl):
            for dz in (1, 7, 3, 5):
                source = y * NZ + lax.rem(z + dz, NZ)
                wait(rows_of(wz, source), w_sem.at[0, source])
                to_sibling(source)

    second(*packs[1])

    for dx in (1, 3, 2):
        @pl.loop(0, NG)
        def _(k):
            place_x = lax.rem(x + dx, NX)
            wait(t_buf.at[place_x, k], a_sem.at[place_x * NG + k])
    wait(t_buf.at[x, g], a_sem.at[lon])
    relay(*packs[0])
    settle(0, wz)

    low256 = lax.broadcasted_iota(jnp.int32, (256, 128), 1) < 64
    zero256 = jnp.zeros((256, 128), BF16)

    def zonal_row(r):
        values = t_buf[:, :, r].astype(F32).reshape(256, 768)
        normed = norm(values, gz[...].reshape(1, 768))
        fields = matmul(normed, wz[...]).astype(BF16)
        q, k, v = fields[:, 0:128], fields[:, 128:256], fields[:, 256:384]
        vq, pad_k = fields[:, 384:512], fields[:, 512:640]
        m0 = matmul(weights_of(q, jnp.where(low256, k, zero256)), v)
        m1 = matmul(weights_of(q, jnp.where(low256, zero256, k)), v)
        m2 = matmul(weights_of(vq, pad_k), vq)
        mz[:, pl.ds(r, 1), :, 0:128] = jnp.where(low256, m0, m1).reshape(32, 1, 8, 128).astype(BF16)
        mz[:, pl.ds(r, 1), :, 128:192] = m2[:, 0:64].reshape(32, 1, 8, 64).astype(BF16)

    def home(low, rows):
        here, there = pl.ds(low, rows), pl.ds(3 * g + low, rows)
        local(mz.at[lon, here], h_buf.at[x, there], b_sem.at[lon]).start()

        @pl.loop(1, NX * NG)
        def _(k):
            to = lax.rem(lon + k, NX * NG)
            remote(mz.at[to, here], h_buf.at[x, there], send.at[10], b_sem.at[lon], lat, to).start()

    zonal_row(0)
    home(0, 1)

    @pl.loop(1, 3)
    def _(r):
        zonal_row(r)

    home(1, 2)

    third(*packs[1])
    first(*packs[2])
    share(*packs[0])
    settle(1, oz)
    second(*packs[2])
    relay(*packs[1])

    @pl.loop(0, NX * NG)
    def _(k):
        wait(h_buf.at[k // NG, pl.ds(3 * lax.rem(k, NG), 3)], b_sem.at[k])

    total = tok[...].astype(F32).reshape(192, 768)
    for i in range(NX):
        mixed = h_buf[i].astype(F32).reshape(192, 192).astype(BF16)
        total += matmul(mixed, oz[192 * i : 192 * i + 192, :])
    by_row = total.astype(BF16)
    ii = lax.broadcasted_iota(jnp.int32, (192, 192), 1)
    jj = lax.broadcasted_iota(jnp.int32, (192, 192), 0)
    turn = jnp.where((ii & 7) * 24 + (ii >> 3) == jj, 1.0, 0.0).astype(BF16)
    by_col = matmul(turn, by_row)
    after[...] = by_col
    s_buf[...] = by_col.reshape(8, 3, 8, 768).astype(BF16)

    local(s_buf.at[z], u_buf.at[yl, z], c_sem.at[lat]).start()
    for dz in (4, 3, 5, 2, 6, 1, 7):
        to = lax.rem(z + dz, NZ)
        remote(s_buf.at[to], u_buf.at[yl, z], send.at[11], c_sem.at[lat], yl * NZ + to, lon).start()
    remote(s_buf.at[z], u_buf.at[yl, z], send.at[12], c_sem.at[lat], pair, lon).start()
    third(*packs[2])
    for dz in (1, 7, 2, 6, 3, 5, 4):
        source = lax.rem(z + dz, NZ)
        block = u_buf.at[yl, source]
        wait(block, c_sem.at[yl * NZ + source])
        remote(block, block, send.at[12], c_sem.at[yl * NZ + source], pair, lon).start()

    share(*packs[1])
    relay(*packs[2])
    settle(2, wm)

    wait(u_buf.at[yl, z], c_sem.at[lat])

    @pl.loop(0, NZ)
    def _(k):
        wait(u_buf.at[1 - yl, k], c_sem.at[(1 - yl) * NZ + k])

    low384 = lax.broadcasted_iota(jnp.int32, (384, 128), 1) < 64
    zero384 = jnp.zeros((384, 128), BF16)
    normed = norm(u_buf[...].astype(F32).reshape(384, 768), gm[...].reshape(1, 768))
    for j in range(3):
        at = 128 * j
        q = matmul(normed, wm[:, at : at + 128]).astype(BF16)
        k = matmul(normed, wm[:, 384 + at : 512 + at]).astype(BF16)
        v = matmul(normed, wm[:, 768 + at : 896 + at]).astype(BF16)
        m0 = matmul(weights_of(q, jnp.where(low384, k, zero384)), v)
        m1 = matmul(weights_of(q, jnp.where(low384, zero384, k)), v)
        mm[j] = jnp.where(low384, m0, m1).reshape(16, 3, 8, 128).astype(BF16)

        there = h2_buf.at[yl, z, :, :, pl.ds(at, 128)]
        local(mm.at[j, lat], there, d_sem.at[lat]).start()

        @pl.loop(1, NY * NZ)
        def _(k):
            to = lax.rem(lat + k, NY * NZ)
            remote(mm.at[j, to], there, send.at[13], d_sem.at[lat], to, lon).start()

    share(*packs[2])
    settle(3, om)

    @pl.loop(0, NY * NZ)
    def _(k):
        wait(h2_buf.at[k // NZ, lax.rem(k, NZ)], d_sem.at[k])

    total = after[...]
    for i in range(NY):
        mixed = h2_buf[i].astype(F32).reshape(192, 384).astype(BF16)
        total += matmul(mixed, om[384 * i : 384 * i + 384, :])
    back = jnp.where((jj & 7) * 24 + (jj >> 3) == ii, 1.0, 0.0).astype(BF16)
    out[...] = matmul(back, total.astype(BF16)).reshape(24, 8, 768).astype(BF16)

    wait(t_buf.at[0, pl.ds(0, NG - 1)], send.at[0])
    wait(t_buf.at[pl.ds(0, 3)], send.at[2])

    @pl.when(active)
    def _():
        wait(wz.at[pl.ds(0, 48 * 15)], send.at[1])

    wait(wz.at[pl.ds(0, 48 * 8)], send.at[3])
    for p, src, dst, s in packs:
        for at, count in ((0, 9), (2, 4), (6, 2)):
            @pl.when(dz_own == at)
            def _():
                wait(dst.at[pl.ds(0, 48 * count)], send.at[s])

        wait(dst.at[pl.ds(0, 48 * 14)], send.at[s + 1])
    wait(mz.at[pl.ds(0, NX * NG - 1)], send.at[10])
    wait(s_buf.at[pl.ds(0, NZ - 1)], send.at[11])
    wait(s_buf, send.at[12])
    wait(mm.at[:, pl.ds(0, NY * NZ - 1)], send.at[13])


def body(tokens, gain_zonal, qkv_zonal, out_zonal, gain_merid, qkv_merid, out_merid):
    return pl.pallas_call(
        kernel,
        out_shape=jax.ShapeDtypeStruct(tokens.shape, BF16),
        in_specs=[pl.BlockSpec(memory_space=pltpu.VMEM)] * 7,
        out_specs=pl.BlockSpec(memory_space=pltpu.VMEM),
        scratch_shapes=[
            pltpu.VMEM((48, 640), BF16),
            pltpu.VMEM((2, 48, 1152), BF16),
            pltpu.VMEM((768, 640), BF16),
            pltpu.VMEM((768, 768), BF16),
            pltpu.VMEM((768, 1152), BF16),
            pltpu.VMEM((768, 768), BF16),
            pltpu.VMEM((NX, NG, 3, 8, 768), BF16),
            pltpu.VMEM((NX, 24, 8, 192), BF16),
            pltpu.VMEM((8, 3, 8, 768), BF16),
            pltpu.VMEM((NY, NZ, 3, 8, 768), BF16),
            pltpu.VMEM((NY, NZ, 3, 8, 384), BF16),
            pltpu.VMEM((NX * NG, 3, 8, 192), BF16),
            pltpu.VMEM((3, NY * NZ, 3, 8, 128), BF16),
            pltpu.VMEM((192, 768), F32),
            pltpu.SemaphoreType.DMA((4, NY * NZ)),
            pltpu.SemaphoreType.DMA((NX * NG,)),
            pltpu.SemaphoreType.DMA((NX * NG,)),
            pltpu.SemaphoreType.DMA((NY * NZ,)),
            pltpu.SemaphoreType.DMA((NY * NZ,)),
            pltpu.SemaphoreType.DMA((14,)),
        ],
        compiler_params=pltpu.CompilerParams(
            collective_id=0, has_side_effects=True, vmem_limit_bytes=56 * 1024 * 1024
        ),
        name="axial",
    )(tokens, gain_zonal, qkv_zonal, out_zonal, gain_merid, qkv_merid, out_merid)


def solution(mesh):
    return jax.shard_map(
        body,
        mesh=mesh,
        in_specs=(
            P("lat", "lon", None),
            P(),
            P("lat", None),
            P("lat", None),
            P(),
            P("lat", None),
            P("lat", None),
        ),
        out_specs=P("lat", "lon", None),
        check_vma=False,
    )
```

```python
import math

import jax
import jax.numpy as jnp
from jax import lax
from jax.experimental import pallas as pl
from jax.experimental.pallas import tpu as pltpu
from jax.sharding import PartitionSpec as P

MESH = pl.DeviceIdType.MESH
F32 = jnp.float32
BF16 = jnp.bfloat16
EPS = 1e-05
SCALE = 0.125 * math.log2(math.e)
NX, NG, NZ, NY = 4, 8, 8, 2


def norm(values, gain):
    factor = lax.rsqrt(jnp.mean(values * values, axis=-1, keepdims=True) + EPS)
    return (values * factor * gain).astype(BF16)


def matmul(a, b):
    return jnp.dot(a, b, preferred_element_type=F32)


def attend(query, keys, values):
    scores = lax.dot_general(query, keys, (((1,), (1,)), ((), ())), preferred_element_type=F32) * SCALE
    powers = jnp.exp2(scores - jnp.max(scores, axis=-1, keepdims=True))
    return matmul(powers.astype(BF16), values) * (1.0 / jnp.sum(powers, axis=-1, keepdims=True))


def kernel(
    tok_hbm, gz_hbm, wz_hbm, oz_hbm, gm_hbm, wm_hbm, om_hbm, out,
    tok, gz, wz_in, oz_in, gm, wm_in, om_in,
    wz_s, wm_s, wz, oz, wm, om, t_buf, h_buf, s_buf, u_buf, h2_buf, mz, mm, after,
    w_sem, a_sem, b_sem, c_sem, d_sem, send, in_sem,
):
    lat, lon = lax.axis_index("lat"), lax.axis_index("lon")
    yl, z = lat // NZ, lax.rem(lat, NZ)
    x, g = lon // NG, lax.rem(lon, NG)
    yh, c = g // 2, lax.rem(g, 2)
    sibling = lon + 1 - 2 * c
    pair = (1 - yl) * NZ + z

    def remote(src, dst, ssem, rsem, to_lat, to_lon):
        return pltpu.make_async_remote_copy(
            src_ref=src, dst_ref=dst, send_sem=ssem, recv_sem=rsem,
            device_id=(to_lat, to_lon), device_id_type=MESH,
        )

    def local(src, dst, sem):
        return pltpu.make_async_copy(src, dst, sem)

    def wait(ref, sem):
        local(ref, ref, sem).wait()

    inputs = [
        local(src, dst, in_sem.at[k])
        for k, (src, dst) in enumerate((
            (wz_hbm, wz_in), (tok_hbm, tok), (wm_hbm, wm_in), (oz_hbm, oz_in), (om_hbm, om_in), (gz_hbm, gz), (gm_hbm, gm),
        ))
    ]
    barrier = pltpu.get_barrier_semaphore()
    for copy in inputs:
        copy.start()

    @pl.loop(1, NX * NG)
    def _(k):
        pl.semaphore_signal(barrier, inc=1, device_id=(lat, lax.rem(lon + k, NX * NG)), device_id_type=MESH)

    @pl.loop(1, NY * NZ)
    def _(k):
        pl.semaphore_signal(barrier, inc=1, device_id=(lax.rem(lat + k, NY * NZ), lon), device_id_type=MESH)

    inputs[0].wait()

    for i in range(NX):
        @pl.when(x == i)
        def _():
            rows = wz_in[...].astype(F32)
            def part(t, low, high):
                return rows[:, 768 * t + 192 * i + low : 768 * t + 192 * i + high]
            wz_s[:, 0:128] = part(0, 0, 128).astype(BF16)
            wz_s[:, 128:256] = part(1, 0, 128).astype(BF16)
            wz_s[:, 256:384] = part(2, 0, 128).astype(BF16)
            wz_s[:, 384:512] = jnp.concatenate([part(2, 128, 192), part(0, 128, 192)], axis=1).astype(BF16)
            wz_s[:, 512:640] = jnp.concatenate([jnp.zeros((48, 64), F32), part(1, 128, 192)], axis=1).astype(BF16)
    inputs[1].wait()
    pl.semaphore_wait(barrier, NX * NG - 1 + NY * NZ - 1)

    def rows_of(dst, source):
        return dst.at[pl.ds(48 * source, 48)]

    def along(p, dst, s, source, src, steps):
        for dz in steps:
            remote(src, rows_of(dst, source), send.at[s], w_sem.at[p, source], yl * NZ + lax.rem(z + dz, NZ), lon).start()

    def emit(p, src, dst, s):
        mine, theirs = (src.at[yl], src.at[1 - yl]) if p == 2 else (src, src)
        remote(theirs, rows_of(dst, lat), send.at[s], w_sem.at[p, lat], pair, lon).start()
        local(mine, rows_of(dst, lat), w_sem.at[p, lat]).start()
        along(p, dst, s, lat, mine, (1, 7, 2, 6))

    active = lax.rem(z, 2) == c

    @pl.when(active)
    def _():
        emit(0, wz_s, wz, 1)

    def place(dy, dc):
        return lax.rem(yh + dy, 4) * 2 + lax.rem(c + dc, 2)

    own_rows = pl.ds(3 * g, 3)
    local(tok.at[own_rows], t_buf.at[x, g], a_sem.at[lon]).start()
    for dy, dc in [(0, 1), (1, 0), (3, 0), (1, 1), (3, 1), (2, 0), (2, 1)]:
        to = place(dy, dc)
        remote(tok.at[pl.ds(3 * to, 3)], t_buf.at[x, g], send.at[0], a_sem.at[lon], lat, x * NG + to).start()

    for copy in inputs[2:]:
        copy.wait()
    for h in range(2):
        for t in range(3):
            wm_s[h, :, 384 * t : 384 * t + 384] = wm_in[:, 768 * t + 384 * h : 768 * t + 384 * h + 384]

    def onward(source, src, steps=(1, 3)):
        for dx in steps:
            remote(src, t_buf.at[x, source], send.at[2], a_sem.at[x * NG + source], lat, lax.rem(x + dx, NX) * NG + g).start()

    onward(g, tok.at[own_rows])

    dz_own = lax.rem(z + NZ - 2 * x - c, NZ)
    source_own, source_far = yl * NZ + 2 * x + c, (1 - yl) * NZ + 2 * x + c
    packs = ((1, oz_in, oz, 4), (2, wm_s, wm, 6), (3, om_in, om, 8))

    def first(p, src, dst, s):
        @pl.when(dz_own == 0)
        def _():
            emit(p, src, dst, s)

    def second(p, src, dst, s):
        @pl.when(dz_own == 0)
        def _():
            wait(rows_of(dst, source_own), w_sem.at[p, source_own])
            wait(rows_of(dst, source_far), w_sem.at[p, source_far])
            along(p, dst, s, source_far, rows_of(dst, source_far), (1, 7, 2, 6))

    def third(p, src, dst, s):
        for at, steps in ((2, (1, 2)), (6, (7,))):
            @pl.when(dz_own == at)
            def _():
                for source in (source_own, source_far):
                    wait(rows_of(dst, source), w_sem.at[p, source])
                    along(p, dst, s, source, rows_of(dst, source), steps)

    def relay(p, src, dst, s):
        for source in (source_own, source_far):
            block = rows_of(dst, source)

            @pl.when((dz_own != 0) & (dz_own != 2) & (dz_own != 6))
            def _():
                wait(block, w_sem.at[p, source])

            for dx in ((1, 3) if p == 1 else (1, 3, 2)):
                remote(block, block, send.at[s + 1], w_sem.at[p, source], lat, lax.rem(x + dx, NX) * NG + g).start()
            remote(block, block, send.at[s + 1], w_sem.at[p, source], lat, sibling).start()

    def taken(p, dst, s, dx, y):
        source = y * NZ + 2 * lax.rem(x + dx, NX) + c
        block = rows_of(dst, source)
        wait(block, w_sem.at[p, source])
        remote(block, block, send.at[s + 1], w_sem.at[p, source], lat, sibling).start()
        return block, source

    def hop(p, src, dst, s):
        for dx, y in ((3, yl), (1, 1 - yl)):
            block, source = taken(p, dst, s, dx, y)
            remote(block, block, send.at[s + 1], w_sem.at[p, source], lat, lax.rem(x + NX - dx, NX) * NG + g).start()

    def share(p, src, dst, s):
        rest = ((3, 1 - yl), (1, yl), (2, yl), (2, 1 - yl))
        for dx, y in (rest if p == 1 else ((3, yl), (1, 1 - yl)) + rest):
            taken(p, dst, s, dx, y)

    def settle(p, dst):
        @pl.loop(0, NZ)
        def _(k):
            source = (k // 4) * NZ + 2 * lax.rem(k, 4) + 1 - c
            wait(rows_of(dst, source), w_sem.at[p, source])

    first(*packs[0])

    def pass_on(pieces):
        for dy, dc in pieces:
            source = place(dy, dc)
            wait(t_buf.at[x, source], a_sem.at[x * NG + source])
            onward(source, t_buf.at[x, source], (1, 3, 2) if dy == 2 else (1, 3))

    def to_sibling(source):
        block = rows_of(wz, source)
        remote(block, block, send.at[3], w_sem.at[0, source], lat, sibling).start()

    def pass_zonal(y):
        @pl.when(active)
        def _():
            for dz, steps in ((6, (1, 2)), (2, (7,))):
                source = y * NZ + lax.rem(z + dz, NZ)
                wait(rows_of(wz, source), w_sem.at[0, source])
                along(0, wz, 1, source, rows_of(wz, source), steps)
                to_sibling(source)

    def cross(dys):
        for dy in dys:
            for dx, dc in ((3, 0), (1, 1)):
                source, from_x = place(dy, dc), lax.rem(x + dx, NX)
                block = t_buf.at[from_x, source]
                wait(block, a_sem.at[from_x * NG + source])
                remote(block, block, send.at[2], a_sem.at[from_x * NG + source], lat, lax.rem(x + NX - dx, NX) * NG + g).start()

    pass_on([(0, 1)])

    @pl.when(active)
    def _():
        wait(rows_of(wz, pair), w_sem.at[0, pair])
        along(0, wz, 1, pair, rows_of(wz, pair), (1, 7, 2, 6))

    second(*packs[0])
    pass_zonal(yl)
    pass_on([(1, 0), (3, 0)])
    cross([0])
    pass_zonal(1 - yl)
    pass_on([(1, 1), (3, 1)])
    third(*packs[0])
    first(*packs[1])
    pass_on([(2, 0), (2, 1)])
    cross([1, 3])

    @pl.when(active)
    def _():
        wait(rows_of(wz, lat), w_sem.at[0, lat])
        to_sibling(lat)
        to_sibling(pair)
        for y in (yl, 1 - yl):
            source = y * NZ + lax.rem(z + 4, NZ)
            wait(rows_of(wz, source), w_sem.at[0, source])
            to_sibling(source)

    @pl.when(jnp.logical_not(active))
    def _():
        for y in (yl, 1 - yl):
            for dz in (1, 7, 3, 5):
                source = y * NZ + lax.rem(z + dz, NZ)
                wait(rows_of(wz, source), w_sem.at[0, source])
                to_sibling(source)

    relay(*packs[0])
    def arrived(dx, source):
        from_x = lax.rem(x + dx, NX)
        wait(t_buf.at[from_x, source], a_sem.at[from_x * NG + source])

    for dy in (0, 1, 3, 2):
        arrived(3, place(dy, 1))
        arrived(1, place(dy, 0))
        if dy == 2:
            arrived(3, place(dy, 0))
            arrived(1, place(dy, 1))
        for dc in (0, 1):
            arrived(2, place(dy, dc))
    wait(t_buf.at[x, g], a_sem.at[lon])
    second(*packs[1])
    settle(0, wz)

    low256 = lax.broadcasted_iota(jnp.int32, (256, 128), 1) < 64
    zero256 = jnp.zeros((256, 128), BF16)

    def zonal_row(r):
        values = t_buf[:, :, r].astype(F32).reshape(256, 768)
        normed = norm(values, gz[...].reshape(1, 768))
        fields = matmul(normed, wz[...]).astype(BF16)
        q, k, v = fields[:, 0:128], fields[:, 128:256], fields[:, 256:384]
        vq, pad_k = fields[:, 384:512], fields[:, 512:640]
        m0 = attend(q, jnp.where(low256, k, zero256), v)
        m1 = attend(q, jnp.where(low256, zero256, k), v)
        m2 = attend(vq, pad_k, vq)
        mz[:, pl.ds(r, 1), :, 0:128] = jnp.where(low256, m0, m1).reshape(32, 1, 8, 128).astype(BF16)
        mz[:, pl.ds(r, 1), :, 128:192] = m2[:, 0:64].reshape(32, 1, 8, 64).astype(BF16)

    def home(low, rows):
        here, there = pl.ds(low, rows), pl.ds(3 * g + low, rows)
        local(mz.at[lon, here], h_buf.at[x, there], b_sem.at[0]).start()

        @pl.loop(1, NX * NG)
        def _(k):
            to = lax.rem(lon + k, NX * NG)
            remote(mz.at[to, here], h_buf.at[x, there], send.at[10], b_sem.at[0], lat, to).start()

    zonal_row(0)
    home(0, 1)
    @pl.loop(1, 3)
    def _(r):
        zonal_row(r)

    home(1, 2)

    hop(*packs[0])
    third(*packs[1])
    first(*packs[2])
    share(*packs[0])
    second(*packs[2])
    settle(1, oz)
    relay(*packs[1])
    third(*packs[2])

    wait(h_buf, b_sem.at[0])

    total = tok[...].astype(F32).reshape(192, 768)
    for i in range(NX):
        mixed = h_buf[i].astype(F32).reshape(192, 192).astype(BF16)
        total += matmul(mixed, oz[192 * i : 192 * i + 192, :])
    by_row = total.astype(BF16)
    ii = lax.broadcasted_iota(jnp.int32, (192, 192), 1)
    jj = lax.broadcasted_iota(jnp.int32, (192, 192), 0)
    turn = jnp.where((ii & 7) * 24 + (ii >> 3) == jj, 1.0, 0.0).astype(BF16)
    by_col = matmul(turn, by_row)
    after[...] = by_col
    s_buf[...] = by_col.reshape(8, 3, 8, 768).astype(BF16)

    local(s_buf.at[z], u_buf.at[yl, z], c_sem.at[lat]).start()
    for dz in (1, 7, 2, 6, 3, 5, 4):
        to = lax.rem(z + dz, NZ)
        remote(s_buf.at[to], u_buf.at[yl, z], send.at[11], c_sem.at[lat], yl * NZ + to, lon).start()
    remote(s_buf.at[z], u_buf.at[yl, z], send.at[12], c_sem.at[lat], pair, lon).start()
    for dz in (1, 7, 2, 6, 3, 5, 4):
        source = lax.rem(z + dz, NZ)
        block = u_buf.at[yl, source]
        wait(block, c_sem.at[yl * NZ + source])
        remote(block, block, send.at[12], c_sem.at[yl * NZ + source], pair, lon).start()

    share(*packs[1])
    relay(*packs[2])
    settle(2, wm)

    wait(u_buf.at[yl, z], c_sem.at[lat])

    @pl.loop(0, NZ)
    def _(k):
        wait(u_buf.at[1 - yl, k], c_sem.at[(1 - yl) * NZ + k])

    low384 = lax.broadcasted_iota(jnp.int32, (384, 128), 1) < 64
    zero384 = jnp.zeros((384, 128), BF16)
    normed = norm(u_buf[...].astype(F32).reshape(384, 768), gm[...].reshape(1, 768))
    fields = matmul(normed, wm[...]).astype(BF16)
    for j in range(3):
        at = 128 * j
        q, k, v = (fields[:, first_at + at : first_at + at + 128] for first_at in (0, 384, 768))
        m0 = attend(q, jnp.where(low384, k, zero384), v)
        m1 = attend(q, jnp.where(low384, zero384, k), v)
        mm[j] = jnp.where(low384, m0, m1).reshape(16, 3, 8, 128).astype(BF16)

        there = h2_buf.at[yl, z, :, :, pl.ds(at, 128)]
        local(mm.at[j, lat], there, d_sem.at[0]).start()

        @pl.loop(1, NY * NZ)
        def _(k):
            to = lax.rem(lat + k, NY * NZ)
            remote(mm.at[j, to], there, send.at[13], d_sem.at[0], to, lon).start()

    share(*packs[2])
    settle(3, om)

    wait(h2_buf, d_sem.at[0])

    total = after[...]
    for i in range(NY):
        mixed = h2_buf[i].astype(F32).reshape(192, 384).astype(BF16)
        total += matmul(mixed, om[384 * i : 384 * i + 384, :])
    back = jnp.where((jj & 7) * 24 + (jj >> 3) == ii, 1.0, 0.0).astype(BF16)
    out[...] = matmul(back, total.astype(BF16)).reshape(24, 8, 768).astype(BF16)

    wait(t_buf.at[0, pl.ds(0, NG - 1)], send.at[0])
    wait(t_buf.at[pl.ds(0, 3)], send.at[2])

    @pl.when(active)
    def _():
        wait(wz.at[pl.ds(0, 48 * 15)], send.at[1])

    wait(wz.at[pl.ds(0, 48 * 8)], send.at[3])
    for p, src, dst, s in packs:
        for at, count in ((0, 9), (2, 4), (6, 2)):
            @pl.when(dz_own == at)
            def _():
                wait(dst.at[pl.ds(0, 48 * count)], send.at[s])

        wait(dst.at[pl.ds(0, 48 * 14)], send.at[s + 1])
    wait(mz.at[pl.ds(0, NX * NG - 1)], send.at[10])
    wait(s_buf.at[pl.ds(0, NZ - 1)], send.at[11])
    wait(s_buf, send.at[12])
    wait(mm.at[:, pl.ds(0, NY * NZ - 1)], send.at[13])


def body(tokens, gain_zonal, qkv_zonal, out_zonal, gain_merid, qkv_merid, out_merid):
    return pl.pallas_call(
        kernel,
        out_shape=pltpu.VMEM(tokens.shape, BF16),
        in_specs=[pl.BlockSpec(memory_space=pltpu.HBM)] * 7,
        out_specs=pl.BlockSpec(memory_space=pltpu.VMEM),
        scratch_shapes=[
            pltpu.VMEM(tokens.shape, BF16),
            pltpu.VMEM(gain_zonal.shape, F32),
            pltpu.VMEM(qkv_zonal.shape, BF16),
            pltpu.VMEM(out_zonal.shape, BF16),
            pltpu.VMEM(gain_merid.shape, F32),
            pltpu.VMEM(qkv_merid.shape, BF16),
            pltpu.VMEM(out_merid.shape, BF16),
            pltpu.VMEM((48, 640), BF16),
            pltpu.VMEM((2, 48, 1152), BF16),
            pltpu.VMEM((768, 640), BF16),
            pltpu.VMEM((768, 768), BF16),
            pltpu.VMEM((768, 1152), BF16),
            pltpu.VMEM((768, 768), BF16),
            pltpu.VMEM((NX, NG, 3, 8, 768), BF16),
            pltpu.VMEM((NX, 24, 8, 192), BF16),
            pltpu.VMEM((8, 3, 8, 768), BF16),
            pltpu.VMEM((NY, NZ, 3, 8, 768), BF16),
            pltpu.VMEM((NY, NZ, 3, 8, 384), BF16),
            pltpu.VMEM((NX * NG, 3, 8, 192), BF16),
            pltpu.VMEM((3, NY * NZ, 3, 8, 128), BF16),
            pltpu.VMEM((192, 768), F32),
            pltpu.SemaphoreType.DMA((4, NY * NZ)),
            pltpu.SemaphoreType.DMA((NX * NG,)),
            pltpu.SemaphoreType.DMA((1,)),
            pltpu.SemaphoreType.DMA((NY * NZ,)),
            pltpu.SemaphoreType.DMA((1,)),
            pltpu.SemaphoreType.DMA((14,)),
            pltpu.SemaphoreType.DMA((7,)),
        ],
        compiler_params=pltpu.CompilerParams(
            collective_id=0, has_side_effects=True, vmem_limit_bytes=66_746_000
        ),
        name="axial",
    )(tokens, gain_zonal, qkv_zonal, out_zonal, gain_merid, qkv_merid, out_merid)


def solution(mesh):
    return jax.shard_map(
        body,
        mesh=mesh,
        in_specs=(
            P("lat", "lon", None),
            P(),
            P("lat", None),
            P("lat", None),
            P(),
            P("lat", None),
            P("lat", None),
        ),
        out_specs=P("lat", "lon", None),
        check_vma=False,
    )
```
